32 devices in a mesh: learner: 8 (over y, x, core), tensor: 4 (over z).
Axes of the slice: x: 2, y: 2, z: 4, core: 2. Of those that a mesh axis runs over, the one named last changes fastest.
Arguments:
- blocks: bfloat16 [64, 128, 4096], P('learner', None, 'tensor'), may hold values from -60 to 60
- seg_ids: int32 [8, 1024], P('learner'), may hold values from 0 to 7, never falling along the last dimension, each value on 1 to 256 neighbouring positions
- dest: int32 [64], replicated, may hold values from 0 to 7, as said below
- slot: int32 [64], replicated, may hold values from 0 to 7, as said below
- norm_gain: bfloat16 [4096], P('tensor'), may hold values from 0.25 to 1.75
- w_query: bfloat16 [4096, 4096], P(None, 'tensor'), may hold values from -2 to 2
- w_keyval: bfloat16 [4096, 2048], P('learner'), may hold values from -2 to 2
Outputs:
- context: bfloat16 [8192, 4096], P('learner', 'tensor')
The draws below stay inside these ranges and needn't reach their ends.
Inputs may be any that keep to these rules, and one draw needn't show every extreme that they name: `dest`: each learner receives exactly 8 blocks; at most 1 of the blocks of one learner go to any one learner, and in every draw some learner sends exactly 1 block to one learner. `slot`: the blocks that one learner receives take the positions 0 to 7 of its packed row, one each.
All inputs are finite; a program needn't handle non-finite values.
Results may differ from the reference program's by a relative error of at most 0.012.
The reference program's roundings to bfloat16 on the way (of `packed`, `normed`, `queries`, `keyval` and `probs`) count: a program that leaves them out, or rounds other values in their place, can miss the bound.
Values may be sent and summed in bfloat16 or wider, within the bound.
A program may use at most 64 MiB of HBM per device.

```python
import math
import jax
import jax.numpy as jnp
import numpy as np
from jax import lax

D = 4096
HEADS = 32
KV_HEADS = 8
HD = 128
BLOCK = 128
BLK_DEV = 8
PACK = 1024
TOKENS = 8192
N_LEARNER = 8


def routing_tables(key):
    base = jax.random.fold_in(key, 11)
    first_key, second_key, third_key = jax.random.split(base, 3)
    outer = jax.random.permutation(first_key, N_LEARNER).astype(jnp.int32)
    inner = jax.random.permutation(second_key, N_LEARNER).astype(jnp.int32)
    turns = jax.random.randint(third_key, (N_LEARNER,), 0, BLK_DEV).astype(jnp.int32)
    counter = jnp.arange(N_LEARNER * BLK_DEV, dtype=jnp.int32)
    source = counter // BLK_DEV
    within = counter % BLK_DEV
    targets = outer[(inner[source] + within) % N_LEARNER]
    places = (within + turns[targets]) % BLK_DEV
    return (targets.astype(jnp.int32), places.astype(jnp.int32))


def draw_dest(key, part):
    return routing_tables(key)[0]


def draw_slot(key, part):
    return routing_tables(key)[1]


def shared_weights(key):
    base = jax.random.fold_in(key, 7)
    query_key, keyval_key = jax.random.split(base, 2)
    w_query = jax.random.normal(query_key, (D, HEADS * HD), jnp.float32) / math.sqrt(D)
    w_keyval = jax.random.normal(keyval_key, (D, 2 * KV_HEADS * HD), jnp.float32) / math.sqrt(D)
    return (jnp.clip(w_query, -2.0, 2.0), jnp.clip(w_keyval, -2.0, 2.0))


def draw_w_query(key, part):
    return shared_weights(key)[0].astype(jnp.bfloat16)


def draw_w_keyval(key, part):
    return shared_weights(key)[1].astype(jnp.bfloat16)


def draw_blocks(key, part):
    base = jax.random.fold_in(key, 3)
    noise_key, scale_key = jax.random.split(base, 2)
    shape = (N_LEARNER * BLK_DEV, BLOCK, D)
    row_scale = jnp.exp(jax.random.uniform(scale_key, (N_LEARNER * BLK_DEV, BLOCK, 1), jnp.float32, 0.0, math.log(10.0)))
    values = jax.random.normal(noise_key, shape, jnp.float32) * row_scale
    return jnp.clip(values, -60.0, 60.0).astype(jnp.bfloat16)


def length_profile(count, total, limit, skew):
    weights = [(1 << 20) // math.isqrt(standing ** skew) + 1 for standing in range(2, count + 1)]
    spare, counts = total - limit - (count - 1), [1] * (count - 1)
    while spare > 0:
        movable = [i for i in range(count - 1) if counts[i] < limit]
        mass, left = sum([weights[i] for i in movable]), spare
        for i in movable:
            extra = min(limit - counts[i], max(1, left * weights[i] // mass), spare)
            counts[i] = counts[i] + extra
            spare = spare - extra
    return np.array([limit] + counts)


def ragged(rng, count, total, limit, lean):
    if count == 2:
        one = jax.random.randint(rng, (), max(1, total - limit), min(limit, total - 1) + 1)
        return jnp.stack([one, total - one])
    sizes = jnp.asarray(length_profile(count, total, limit, lean), jnp.int32)
    couples = (count - 1) // 2
    source_of, sink = sizes[1:1 + 2 * couples:2], sizes[2:2 + 2 * couples:2]
    room = jnp.minimum(source_of - 1, limit - sink)
    moved = jax.random.randint(jax.random.fold_in(rng, 1), (couples,), 0, 1 << 20) % (room + 1)
    sizes = sizes.at[1:1 + 2 * couples:2].set(source_of - moved).at[2:2 + 2 * couples:2].set(sink + moved)
    return sizes[jax.random.permutation(jax.random.fold_in(rng, 2), count)]


def setup_inputs(seed: int = 0) -> dict:
    key_list = jax.random.split(jax.random.key(seed), 8)
    blocks = draw_blocks(jax.random.fold_in(key_list[7], 71), 0)
    seg_ids = jax.vmap(lambda own: jnp.searchsorted(jnp.cumsum(ragged(own, 8, PACK, PACK // 4, 2)), jnp.arange(PACK), side="right"))(jax.random.split(key_list[1], N_LEARNER)).reshape((N_LEARNER, PACK)).astype(jnp.int32)
    dest = draw_dest(jax.random.fold_in(key_list[7], 71), 0)
    slot = draw_slot(jax.random.fold_in(key_list[7], 71), 0)
    norm_gain = jnp.clip(1.0 + 0.15 * jax.random.normal(key_list[4], (D,), jnp.float32), 0.25, 1.75).astype(jnp.bfloat16)
    w_query = draw_w_query(jax.random.fold_in(key_list[7], 71), 0)
    w_keyval = draw_w_keyval(jax.random.fold_in(key_list[7], 71), 0)
    return {"blocks": blocks, "seg_ids": seg_ids, "dest": dest, "slot": slot, "norm_gain": norm_gain, "w_query": w_query, "w_keyval": w_keyval}


def reference(blocks, seg_ids, dest, slot, norm_gain, w_query, w_keyval):
    positions = (dest * BLK_DEV + slot).astype(jnp.int32)
    packed = jnp.zeros_like(blocks).at[positions].set(blocks)
    packed = packed.reshape(N_LEARNER, BLK_DEV * BLOCK, D)
    group = HEADS // KV_HEADS

    def one_shard(shard_item):
        shard_rows, segment = shard_item
        widened = shard_rows.astype(jnp.float32)
        mean_sq = lax.optimization_barrier(jnp.mean(widened * widened, axis=-1, keepdims=True))
        normed = (widened * lax.rsqrt(mean_sq + 1e-05) * norm_gain.astype(jnp.float32)).astype(jnp.bfloat16)
        queries = jnp.dot(normed, w_query, preferred_element_type=jnp.float32).astype(jnp.bfloat16)
        keyval = jnp.dot(normed, w_keyval, preferred_element_type=jnp.float32).astype(jnp.bfloat16)
        length = shard_rows.shape[0]
        query_heads = queries.reshape(length, HEADS, HD).astype(jnp.float32)
        keyval_split = keyval.reshape(length, KV_HEADS, 2, HD).astype(jnp.float32)
        key_heads = jnp.repeat(keyval_split[:, :, 0], group, axis=1)
        value_heads = jnp.repeat(keyval_split[:, :, 1], group, axis=1)
        scores = jnp.einsum('qhd,khd->hqk', query_heads, key_heads) / math.sqrt(HD)
        index = jnp.arange(length, dtype=jnp.int32)
        allowed = (segment[:, None] == segment[None, :]) & (index[None, :] <= index[:, None])
        masked = jnp.where(allowed[None], scores, -1e+30)
        row_max = lax.optimization_barrier(jnp.max(masked, axis=-1, keepdims=True))
        exponent = jnp.where(allowed[None], jnp.exp(masked - row_max), 0.0)
        probs = (exponent / lax.optimization_barrier(jnp.sum(exponent, axis=-1, keepdims=True))).astype(jnp.bfloat16)
        context = jnp.einsum('hqk,khd->qhd', probs.astype(jnp.float32), value_heads)
        return context.astype(jnp.bfloat16).reshape(length, HEADS * HD)
    result = lax.map(one_shard, (packed, seg_ids))
    return result.reshape(TOKENS, HEADS * HD)
```

```python
import functools
import math

import jax
import jax.numpy as jnp
from jax import lax
from jax.experimental import pallas as pl
from jax.experimental.pallas import tpu as pltpu
from jax.sharding import PartitionSpec as P

D = 4096
HEADS = 32
KV_HEADS = 8
HD = 128
MAX_RUN = 256
MESH = pl.DeviceIdType.MESH


def on_device_general(blocks, seg_ids, dest, slot, norm_gain, w_query, w_keyval):
    learners = lax.axis_size("learner")
    own_index = lax.axis_index("learner")
    blk_dev, block_len, features = blocks.shape
    capacity = (blk_dev + learners - 1) // learners
    targets = dest.reshape(learners, blk_dev)
    places = slot.reshape(learners, blk_dev)
    block_ids = jnp.arange(blk_dev, dtype=jnp.int32)
    earlier = block_ids[None, :] < block_ids[:, None]
    same_target = targets[:, :, None] == targets[:, None, :]
    ranks = jnp.sum(jnp.where(same_target & earlier[None], 1, 0), axis=2).astype(jnp.int32)
    own_targets = lax.dynamic_index_in_dim(targets, own_index, 0, keepdims=False)
    own_ranks = lax.dynamic_index_in_dim(ranks, own_index, 0, keepdims=False)
    send_slots = own_targets * capacity + own_ranks
    slot_range = jnp.arange(learners * capacity, dtype=jnp.int32)
    send_table = (send_slots[None, :] == slot_range[:, None]).astype(jnp.bfloat16)
    outgoing = jnp.dot(send_table, blocks.reshape(blk_dev, -1), preferred_element_type=jnp.float32)
    outgoing = outgoing.astype(jnp.bfloat16).reshape(learners * capacity, block_len, features)
    incoming = lax.all_to_all(outgoing, "learner", split_axis=0, concat_axis=0, tiled=True)
    arrive = (targets == own_index).reshape(-1)
    source_slots = (jnp.arange(learners, dtype=jnp.int32)[:, None] * capacity + ranks).reshape(-1)
    place_hot = ((places.reshape(-1)[:, None] == block_ids[None, :]) & arrive[:, None]).astype(
        jnp.float32
    )
    source_hot = (source_slots[:, None] == slot_range[None, :]).astype(jnp.float32)
    receive_table = jnp.dot(place_hot.T, source_hot).astype(jnp.bfloat16)
    local = jnp.dot(
        receive_table, incoming.reshape(learners * capacity, -1), preferred_element_type=jnp.float32
    )
    local = local.astype(jnp.bfloat16).reshape(blk_dev * block_len, features)
    heads_dev = w_query.shape[1] // HD
    per_group = HEADS // KV_HEADS
    groups_dev = max(1, heads_dev // per_group)
    first_group = lax.axis_index("tensor") * heads_dev // per_group
    kv_columns = lax.dynamic_slice_in_dim(w_keyval, first_group * 2 * HD, groups_dev * 2 * HD, 1)
    kv_weight = lax.all_gather(kv_columns, "learner", axis=0, tiled=True)
    own_squares = jnp.einsum("rd,rd->r", local, local, preferred_element_type=jnp.float32)
    squares = lax.psum(own_squares, "tensor")
    inverse_rms = lax.rsqrt(squares / D + 1e-05)
    normed_part = (
        local.astype(jnp.float32) * inverse_rms[:, None] * norm_gain.astype(jnp.float32)[None, :]
    ).astype(jnp.bfloat16)
    part_rows = lax.all_gather(normed_part, "tensor", axis=1, tiled=True)
    query_sum = jnp.dot(part_rows, w_query, preferred_element_type=jnp.float32)
    keyval_sum = jnp.dot(part_rows, kv_weight, preferred_element_type=jnp.float32)
    queries = query_sum.astype(jnp.bfloat16)
    keyval = keyval_sum.astype(jnp.bfloat16)
    row_count = queries.shape[0]
    places_own = jnp.arange(row_count // block_len, dtype=jnp.int32)
    qkv = jnp.concatenate([queries, keyval], axis=1)
    qkv = qkv.reshape(row_count // block_len, block_len, -1)
    return attention(qkv, seg_ids, places_own, heads_dev, groups_dev)


def bit_flip(value, mask):
    out = value
    bit = 1
    while bit <= mask:
        if mask & bit:
            out = out + bit - 2 * bit * lax.rem(lax.div(value, bit), 2)
        bit *= 2
    return out


def gather_project_kernel(
    order, n, nt, own_cols, kv_cols,
    dest_ref, blocks_ref, gain_ref, wq_ref, wkv_ref, out_ref,
    staged, sorted_, gath, gains, weight, normed, projected,
    load_sem, wq_sem, kvl_sem, a2a_s, a2a_r, kv_s, kv_r, g_s, g_r, z_s, z_r, out_sem,
):
    me = lax.axis_index("learner")
    t = lax.axis_index("tensor")
    features = blocks_ref.shape[2]
    rows = wkv_ref.shape[0]

    load = pltpu.make_async_copy(blocks_ref, staged, load_sem)
    load.start()
    kv_mine = weight.at[pl.ds(pl.multiple_of(me * rows, 128), rows), pl.ds(own_cols, kv_cols)]
    kv_local = pltpu.make_async_copy(
        wkv_ref.at[:, pl.ds(pl.multiple_of(t * kv_cols, 128), kv_cols)], kv_mine, kvl_sem
    )
    kv_local.start()
    wq_load = pltpu.make_async_copy(wq_ref, weight.at[:, pl.ds(0, own_cols)], wq_sem)
    wq_load.start()

    peers = [bit_flip(me, d) for d in order]
    barrier = pltpu.get_barrier_semaphore()
    for k in range(1, n):
        pl.semaphore_signal(barrier, inc=1, device_id=(peers[k], t), device_id_type=MESH)
    for j in range(1, nt):
        pl.semaphore_signal(
            barrier, inc=1, device_id=(me, lax.rem(t + j, nt)), device_id_type=MESH
        )

    gains[t] = gain_ref[...]
    load.wait()
    for k in range(n):
        pick = jnp.int32(0)
        for b in range(n):
            pick = jnp.where(dest_ref[me * n + b] == peers[k], b, pick)
        if k == 0:
            gath[t, 0] = staged[pick]
        else:
            sorted_[k] = staged[pick]
    pl.semaphore_wait(barrier, n - 1 + nt - 1)

    def swap(k):
        return pltpu.make_async_remote_copy(
            src_ref=sorted_.at[k], dst_ref=gath.at[t, k], send_sem=a2a_s.at[k],
            recv_sem=a2a_r.at[k], device_id=(peers[k], t), device_id_type=MESH,
        )

    def kv_move(k):
        return pltpu.make_async_remote_copy(
            src_ref=kv_mine, dst_ref=kv_mine, send_sem=kv_s.at[k],
            recv_sem=kv_r.at[k], device_id=(peers[k], t), device_id_type=MESH,
        )

    def gain_move(j):
        return pltpu.make_async_remote_copy(
            src_ref=gains.at[t], dst_ref=gains.at[t], send_sem=g_s.at[j],
            recv_sem=g_r.at[j], device_id=(me, lax.rem(t + j, nt)), device_id_type=MESH,
        )

    def hop(way, s, k):
        return pltpu.make_async_remote_copy(
            src_ref=gath.at[s, k], dst_ref=gath.at[s, k], send_sem=z_s.at[way, s, k],
            recv_sem=z_r.at[s, k], device_id=(me, t + 1 if way else t - 1),
            device_id_type=MESH,
        )

    for k in range(1, n):
        swap(k).start()
    for j in range(1, nt):
        gain_move(j).start()

    def send_own(k):
        @pl.when(t < nt - 1)
        def _():
            hop(1, t, k).start()

        @pl.when(t > 0)
        def _():
            hop(0, t, k).start()

    send_own(0)
    kv_local.wait()
    for k in range(1, n):
        kv_move(k).start()
    for k in range(1, n):
        swap(k).wait_recv()
        send_own(k)

    for h in range(1, nt - 1):
        def forward(k, carry, h=h):
            @pl.when((t - h >= 0) & (t < nt - 1))
            def _():
                copy = hop(1, t - h, k)
                copy.wait_recv()
                copy.start()

            @pl.when((t + h < nt) & (t > 0))
            def _():
                copy = hop(0, t + h, k)
                copy.wait_recv()
                copy.start()

            return carry

        lax.fori_loop(0, n, forward, 0)

    wq_load.wait()
    for j in range(1, nt):
        gain_move(j).wait_recv()
    for k in range(1, n):
        kv_move(k).wait_recv()

    width = weight.shape[1]
    tile = 512

    def out_copy(k):
        return pltpu.make_async_copy(projected.at[k], out_ref.at[k], out_sem.at[k])

    def project(k, carry):
        for s in range(nt):
            @pl.when(((t == nt - 1) & (s < t)) | ((t == 0) & (s > t)))
            def _(s=s):
                hop(1, s, k).wait_recv()

        total = jnp.zeros((gath.shape[2], 1), jnp.float32)
        for s in range(nt):
            wide = gath[s, k].astype(jnp.float32)
            total = total + jnp.sum(wide * wide, axis=1, keepdims=True)
        inverse = lax.rsqrt(total / (features * nt) + 1e-05)
        for s in range(nt):
            wide = gath[s, k].astype(jnp.float32)
            scaled = wide * inverse * gains[s].astype(jnp.float32)
            normed[:, s * features:(s + 1) * features] = scaled.astype(jnp.bfloat16)

        for c in range(0, width, tile):
            projected[k, :, c:c + tile] = jnp.dot(
                normed[...], weight[:, c:c + tile], preferred_element_type=jnp.float32
            ).astype(jnp.bfloat16)
        out_copy(k).start()
        return carry

    lax.fori_loop(0, n, project, 0)

    for k in range(1, n):
        swap(k).wait_send()
        kv_move(k).wait_send()
    for j in range(1, nt):
        gain_move(j).wait_send()
    for h in range(nt - 1):
        def drain(k, carry, h=h):
            @pl.when((t - h >= 0) & (t < nt - 1))
            def _():
                hop(1, t - h, k).wait_send()

            @pl.when((t + h < nt) & (t > 0))
            def _():
                hop(0, t + h, k).wait_send()

            return carry

        lax.fori_loop(0, n, drain, 0)
    for k in range(n):
        out_copy(k).wait()


def attention_kernel(heads_dev, groups_dev, back, places_ref, seg_ref, qkv_ref, out_ref, held, segs, sem):
    r = pl.program_id(0)
    count, length, _ = qkv_ref.shape
    span = (back + 1) * length

    def fetch(k):
        place = places_ref[k]
        return pltpu.make_async_copy(qkv_ref.at[k], held.at[place + back], sem.at[place])

    @pl.when(r == 0)
    def _():
        for k in range(count):
            fetch(k).start()
        held[0:back] = jnp.zeros((back,) + held.shape[1:], held.dtype)
        for k in range(back):
            segs[k] = jnp.full((1, length), -1, jnp.int32)
        for k in range(count):
            segs[back + k] = seg_ref[:, k * length:(k + 1) * length]

    pltpu.make_async_copy(qkv_ref.at[0], held.at[r + back], sem.at[r]).wait()
    own_seg = jnp.broadcast_to(segs[r + back], (length, length)).T
    same = [own_seg == segs[r + b] for b in range(back + 1)]
    rows_i = lax.broadcasted_iota(jnp.int32, (length, length), 0)
    cols_i = lax.broadcasted_iota(jnp.int32, (length, length), 1)
    same[back] = same[back] & (cols_i <= rows_i)
    bias = jnp.concatenate([jnp.where(m, 0.0, -1e30) for m in same], axis=1)
    stack = heads_dev // groups_dev
    bias = jnp.concatenate([bias] * stack, axis=0)
    base = heads_dev * HD
    for g in range(groups_dev):
        first = g * stack
        query = jnp.concatenate(
            [held[r + back, :, (first + i) * HD:(first + i + 1) * HD] for i in range(stack)], axis=0
        )
        k_at = base + 2 * g * HD
        key = jnp.concatenate([held[r + b, :, k_at:k_at + HD] for b in range(back + 1)], axis=0)
        value = jnp.concatenate(
            [held[r + b, :, k_at + HD:k_at + 2 * HD] for b in range(back + 1)], axis=0
        )
        scores = lax.dot_general(
            query, key, (((1,), (1,)), ((), ())), preferred_element_type=jnp.float32
        )
        masked = scores * (1.0 / math.sqrt(HD)) + bias
        top = jnp.max(masked, axis=1, keepdims=True)
        power = jnp.exp(masked - top)
        probs = (power * (1.0 / jnp.sum(power, axis=1, keepdims=True))).astype(jnp.bfloat16)
        context = jnp.dot(probs, value, preferred_element_type=jnp.float32).astype(jnp.bfloat16)
        for i in range(stack):
            out_ref[:, (first + i) * HD:(first + i + 1) * HD] = context[i * length:(i + 1) * length]


def attention(qkv, seg_ids, places, heads_dev, groups_dev):
    count, length, width = qkv.shape
    back = (MAX_RUN - 1 + length - 1) // length
    return pl.pallas_call(
        functools.partial(attention_kernel, heads_dev, groups_dev, back),
        grid_spec=pltpu.PrefetchScalarGridSpec(
            num_scalar_prefetch=1,
            grid=(count,),
            in_specs=[
                pl.BlockSpec(memory_space=pltpu.VMEM),
                pl.BlockSpec(memory_space=pl.ANY),
            ],
            out_specs=pl.BlockSpec((length, heads_dev * HD), lambda r, places: (r, 0)),
            scratch_shapes=[
                pltpu.VMEM((count + back, length, width), jnp.bfloat16),
                pltpu.VMEM((count + back, 1, length), jnp.int32),
                pltpu.SemaphoreType.DMA((count,)),
            ],
        ),
        out_shape=jax.ShapeDtypeStruct((count * length, heads_dev * HD), jnp.bfloat16),
        compiler_params=pltpu.CompilerParams(dimension_semantics=("arbitrary",)),
        name="attention",
    )(places, seg_ids, qkv)


def on_device_pairwise(n, nt, blocks, seg_ids, dest, slot, norm_gain, w_query, w_keyval):
    order = sorted(range(n), key=lambda d: (bin(d).count("1"), d))
    own_index = lax.axis_index("learner")
    blk_dev, block_len, features = blocks.shape
    heads_dev = w_query.shape[1] // HD
    groups_dev = heads_dev // (HEADS // KV_HEADS)
    own_cols = w_query.shape[1]
    kv_cols = groups_dev * 2 * HD
    width = own_cols + kv_cols
    rows = w_query.shape[0]
    any_spec = pl.BlockSpec(memory_space=pl.ANY)
    qkv = pl.pallas_call(
        functools.partial(gather_project_kernel, order, n, nt, own_cols, kv_cols),
        out_shape=jax.ShapeDtypeStruct((n, block_len, width), jnp.bfloat16),
        in_specs=[
            pl.BlockSpec(memory_space=pltpu.SMEM),
            any_spec,
            pl.BlockSpec(memory_space=pltpu.VMEM),
            any_spec,
            any_spec,
        ],
        out_specs=any_spec,
        scratch_shapes=[
            pltpu.VMEM((n, block_len, features), jnp.bfloat16),
            pltpu.VMEM((n, block_len, features), jnp.bfloat16),
            pltpu.VMEM((nt, n, block_len, features), jnp.bfloat16),
            pltpu.VMEM((nt, 1, features), jnp.float32),
            pltpu.VMEM((rows, width), jnp.bfloat16),
            pltpu.VMEM((block_len, rows), jnp.bfloat16),
            pltpu.VMEM((n, block_len, width), jnp.bfloat16),
            pltpu.SemaphoreType.DMA,
            pltpu.SemaphoreType.DMA,
            pltpu.SemaphoreType.DMA,
            pltpu.SemaphoreType.DMA((n,)),
            pltpu.SemaphoreType.DMA((n,)),
            pltpu.SemaphoreType.DMA((n,)),
            pltpu.SemaphoreType.DMA((n,)),
            pltpu.SemaphoreType.DMA((nt,)),
            pltpu.SemaphoreType.DMA((nt,)),
            pltpu.SemaphoreType.DMA((2, nt, n)),
            pltpu.SemaphoreType.DMA((nt, n)),
            pltpu.SemaphoreType.DMA((n,)),
        ],
        compiler_params=pltpu.CompilerParams(
            collective_id=0, has_side_effects=True, vmem_limit_bytes=60000 * 1024
        ),
        name="gather_project",
    )(dest, blocks, norm_gain.astype(jnp.float32)[None, :], w_query, w_keyval)
    targets = dest.reshape(n, blk_dev)
    arriving = jnp.sum(jnp.where(targets == own_index, slot.reshape(n, blk_dev), 0), axis=1)
    sources = own_index ^ jnp.array(order, jnp.int32)
    places = jnp.sum(
        jnp.where(sources[:, None] == jnp.arange(n, dtype=jnp.int32)[None, :], arriving[None, :], 0),
        axis=1,
    ).astype(jnp.int32)
    return attention(qkv, seg_ids, places, heads_dev, groups_dev)


def solution(mesh):
    n, nt = mesh.shape["learner"], mesh.shape["tensor"]

    def on_device(blocks, seg_ids, dest, slot, norm_gain, w_query, w_keyval):
        args = (blocks, seg_ids, dest, slot, norm_gain, w_query, w_keyval)
        whole_groups = w_query.shape[1] % (HD * HEADS // KV_HEADS) == 0
        if blocks.shape[0] == n and n & (n - 1) == 0 and nt > 1 and whole_groups:
            return on_device_pairwise(n, nt, *args)
        return on_device_general(*args)

    return jax.shard_map(
        on_device,
        mesh=mesh,
        in_specs=(
            P("learner", None, "tensor"),
            P("learner", None),
            P(),
            P(),
            P("tensor"),
            P(None, "tensor"),
            P("learner", None),
        ),
        out_specs=P("learner", "tensor"),
        check_vma=False,
    )
```

```python
import functools
import math

import jax
import jax.numpy as jnp
from jax import lax
from jax.experimental import pallas as pl
from jax.experimental.pallas import tpu as pltpu
from jax.sharding import PartitionSpec as P

D = 4096
HEADS = 32
KV_HEADS = 8
HD = 128
MAX_RUN = 256
MESH = pl.DeviceIdType.MESH


def on_device_general(blocks, seg_ids, dest, slot, norm_gain, w_query, w_keyval):
    learners = lax.axis_size("learner")
    own_index = lax.axis_index("learner")
    blk_dev, block_len, features = blocks.shape
    capacity = (blk_dev + learners - 1) // learners
    targets = dest.reshape(learners, blk_dev)
    places = slot.reshape(learners, blk_dev)
    block_ids = jnp.arange(blk_dev, dtype=jnp.int32)
    earlier = block_ids[None, :] < block_ids[:, None]
    same_target = targets[:, :, None] == targets[:, None, :]
    ranks = jnp.sum(jnp.where(same_target & earlier[None], 1, 0), axis=2).astype(jnp.int32)
    own_targets = lax.dynamic_index_in_dim(targets, own_index, 0, keepdims=False)
    own_ranks = lax.dynamic_index_in_dim(ranks, own_index, 0, keepdims=False)
    send_slots = own_targets * capacity + own_ranks
    slot_range = jnp.arange(learners * capacity, dtype=jnp.int32)
    send_table = (send_slots[None, :] == slot_range[:, None]).astype(jnp.bfloat16)
    outgoing = jnp.dot(send_table, blocks.reshape(blk_dev, -1), preferred_element_type=jnp.float32)
    outgoing = outgoing.astype(jnp.bfloat16).reshape(learners * capacity, block_len, features)
    incoming = lax.all_to_all(outgoing, "learner", split_axis=0, concat_axis=0, tiled=True)
    arrive = (targets == own_index).reshape(-1)
    source_slots = (jnp.arange(learners, dtype=jnp.int32)[:, None] * capacity + ranks).reshape(-1)
    place_hot = ((places.reshape(-1)[:, None] == block_ids[None, :]) & arrive[:, None]).astype(
        jnp.float32
    )
    source_hot = (source_slots[:, None] == slot_range[None, :]).astype(jnp.float32)
    receive_table = jnp.dot(place_hot.T, source_hot).astype(jnp.bfloat16)
    local = jnp.dot(
        receive_table, incoming.reshape(learners * capacity, -1), preferred_element_type=jnp.float32
    )
    local = local.astype(jnp.bfloat16).reshape(blk_dev * block_len, features)
    heads_dev = w_query.shape[1] // HD
    per_group = HEADS // KV_HEADS
    groups_dev = max(1, heads_dev // per_group)
    first_group = lax.axis_index("tensor") * heads_dev // per_group
    kv_columns = lax.dynamic_slice_in_dim(w_keyval, first_group * 2 * HD, groups_dev * 2 * HD, 1)
    kv_weight = lax.all_gather(kv_columns, "learner", axis=0, tiled=True)
    own_squares = jnp.einsum("rd,rd->r", local, local, preferred_element_type=jnp.float32)
    squares = lax.psum(own_squares, "tensor")
    inverse_rms = lax.rsqrt(squares / D + 1e-05)
    normed_part = (
        local.astype(jnp.float32) * inverse_rms[:, None] * norm_gain.astype(jnp.float32)[None, :]
    ).astype(jnp.bfloat16)
    part_rows = lax.all_gather(normed_part, "tensor", axis=1, tiled=True)
    query_sum = jnp.dot(part_rows, w_query, preferred_element_type=jnp.float32)
    keyval_sum = jnp.dot(part_rows, kv_weight, preferred_element_type=jnp.float32)
    queries = query_sum.astype(jnp.bfloat16)
    keyval = keyval_sum.astype(jnp.bfloat16)
    row_count = queries.shape[0]
    places_own = jnp.arange(row_count // block_len, dtype=jnp.int32)
    qkv = jnp.concatenate([queries, keyval], axis=1)
    qkv = qkv.reshape(row_count // block_len, block_len, -1)
    return attention(qkv, seg_ids, places_own, heads_dev, groups_dev)


def bit_flip(value, mask):
    out = value
    bit = 1
    while bit <= mask:
        if mask & bit:
            out = out + bit - 2 * bit * lax.rem(lax.div(value, bit), 2)
        bit *= 2
    return out


def gather_project_kernel(
    order, n, nt, own_cols, kv_cols,
    dest_ref, blocks_ref, gain_ref, wq_ref, wkv_ref, out_ref,
    staged, sorted_, gath, gains, weight, weight_end, normed, projected, part, scales,
    load_sem, wq_sem, kvl_sem, kvx_l, a2a_s, a2a_r, kv_s, kv_f, kv_r, kvx_s, kvx_f, kvx_r,
    wx_s, wx_r, g_s, g_r, z_s, z_r, p_s, p_r, i_s, i_r, out_sem,
):
    me = lax.axis_index("learner")
    t = lax.axis_index("tensor")
    features = blocks_ref.shape[2]
    length = blocks_ref.shape[1]
    rows = wkv_ref.shape[0]
    width = weight.shape[2]
    half_rows = weight_end.shape[0]
    core = lax.rem(me, 2)
    mid = (t > 0) & (t < nt - 1)
    end = (t == 0) | (t == nt - 1)
    side = lax.div(t, 2)
    far = 1 - side
    end_t = jnp.where(side == 0, 0, nt - 1)
    mid_t = jnp.where(side == 0, 1, nt - 2)
    other_mid = jnp.where(side == 0, nt - 2, 1)
    other_end = jnp.where(side == 0, nt - 1, 0)
    peer_of = [bit_flip(me, d) for d in range(n)]
    peers = [peer_of[d] for d in order]
    evens = range(2, n, 2)

    load = pltpu.make_async_copy(blocks_ref, staged, load_sem)
    load.start()

    def slab(owner):
        place = pl.multiple_of(lax.rem(owner, n // 2) * rows, 128)
        return weight.at[lax.div(owner, n // 2), pl.ds(place, rows), pl.ds(own_cols, kv_cols)]

    def far_slab(owner):
        place = lax.rem(owner, n // 2)
        return weight_end.at[
            pl.ds(pl.multiple_of(place * rows, 128), rows), pl.ds(own_cols, kv_cols)
        ]

    def in_far(d):
        return lax.div(peer_of[d], n // 2) == far

    kv_local = pltpu.make_async_copy(
        wkv_ref.at[:, pl.ds(pl.multiple_of(t * kv_cols, 128), kv_cols)], slab(me), kvl_sem
    )
    kv_local.start()

    def kvx_local():
        return pltpu.make_async_copy(
            wkv_ref.at[:, pl.ds(pl.multiple_of(end_t * kv_cols, 128), kv_cols)],
            far_slab(me), kvx_l,
        )

    @pl.when(mid & in_far(0))
    def _():
        kvx_local().start()

    wq_loads = [
        pltpu.make_async_copy(
            wq_ref.at[pl.ds(h * half_rows, half_rows), :],
            weight.at[h, :, pl.ds(0, own_cols)], wq_sem.at[h],
        )
        for h in range(2)
    ]
    for copy in wq_loads:
        copy.start()

    barrier = pltpu.get_barrier_semaphore()
    for k in range(1, n):
        pl.semaphore_signal(barrier, inc=1, device_id=(peers[k], t), device_id_type=MESH)
    for j in range(1, nt):
        pl.semaphore_signal(
            barrier, inc=1, device_id=(me, lax.rem(t + j, nt)), device_id_type=MESH
        )

    gains[t] = gain_ref[...]
    load.wait()
    for k in range(n):
        pick = jnp.int32(0)
        for b in range(n):
            pick = jnp.where(dest_ref[me * n + b] == peers[k], b, pick)
        if k == 0:
            gath[t, 0] = staged[pick]
        else:
            sorted_[k] = staged[pick]
    pl.semaphore_wait(barrier, n - 1 + nt - 1)

    def remote(src, dst, send, recv, device):
        return pltpu.make_async_remote_copy(
            src_ref=src, dst_ref=dst, send_sem=send, recv_sem=recv,
            device_id=device, device_id_type=MESH,
        )

    def swap(k):
        return remote(sorted_.at[k], gath.at[t, k], a2a_s.at[k], a2a_r.at[k], (peers[k], t))

    def kv_direct(d):
        return remote(slab(me), slab(me), kv_s.at[d], kv_r.at[d], (peer_of[d], t))

    def kv_across(d):
        held = slab(peer_of[d])
        return remote(held, held, kv_f.at[d], kv_r.at[d + 1], (peer_of[1], t))

    def kvx_direct(d):
        return remote(far_slab(me), far_slab(me), kvx_s.at[d], kvx_r.at[d], (peer_of[d], t))

    def kvx_across(d):
        held = far_slab(peer_of[d])
        return remote(held, held, kvx_f.at[d], kvx_r.at[d + 1], (peer_of[1], t))

    def wx_rows(c):
        count = half_rows // 2
        return weight_end.at[pl.ds(pl.multiple_of(c * count, 128), count), pl.ds(0, own_cols)]

    def wx_out():
        count = half_rows // 2
        first = pl.multiple_of(far * half_rows + core * count, 128)
        return remote(
            wq_ref.at[pl.ds(first, count), :], wx_rows(core), wx_s.at[0], wx_r.at[0], (me, mid_t)
        )

    def wx_across():
        held = wx_rows(core)
        return remote(held, held, wx_s.at[1], wx_r.at[1], (peer_of[1], t))

    def gain_move(j):
        return remote(gains.at[t], gains.at[t], g_s.at[j], g_r.at[j], (me, lax.rem(t + j, nt)))

    def hop(way, s, k):
        held = gath.at[s, k]
        return remote(
            held, held, z_s.at[way, s, k], z_r.at[s, k], (me, t + 1 if way else t - 1)
        )

    def part_move(k):
        return remote(part.at[k], part.at[k], p_s.at[k], p_r.at[k], (me, end_t))

    def scale_move(k):
        return remote(scales.at[k], scales.at[k], i_s.at[k], i_r.at[k], (me, end_t))

    @pl.when(end)
    def _():
        wx_out().start()

    for k in range(1, n):
        swap(k).start()
    for j in range(1, nt):
        gain_move(j).start()

    def send_own(k):
        @pl.when(t < nt - 1)
        def _():
            hop(1, t, k).start()

        @pl.when(t > 0)
        def _():
            hop(0, t, k).start()

    send_own(0)

    @pl.when(mid & in_far(0))
    def _():
        kvx_local().wait()
        for d in evens:
            kvx_direct(d).start()
        kvx_across(0).start()

    kv_local.wait()
    for d in evens:
        kv_direct(d).start()
    kv_across(0).start()
    for k in range(1, n):
        swap(k).wait_recv()
        send_own(k)
    for j in range(1, nt):
        gain_move(j).wait_recv()

    tile = 512

    def out_copy(k):
        return pltpu.make_async_copy(projected.at[k], out_ref.at[k], out_sem.at[k])

    def relay_kv():
        for d in evens:
            kv_direct(d).wait_recv()
            kv_across(d).start()
        for d in range(0, n, 2):
            kv_across(d).wait_recv()

    batch = n // 2

    def own_project(q):
        group = pl.ds(q * batch, batch)
        for c in range(0, width, tile):
            low = jnp.dot(
                normed[0, group].reshape(batch * length, half_rows), weight[0, :, c:c + tile],
                preferred_element_type=jnp.float32,
            )
            high = jnp.dot(
                normed[1, group].reshape(batch * length, half_rows), weight[1, :, c:c + tile],
                preferred_element_type=jnp.float32,
            )
            projected[group, :, c:c + tile] = (
                (low + high).astype(jnp.bfloat16).reshape(batch, length, tile)
            )
        for i in range(batch):
            out_copy(q * batch + i).start()

    def mid_step(k):
        @pl.when(t == 1)
        def _():
            copy = hop(1, end_t, k)
            copy.wait_recv()
            copy.start()

        @pl.when(t == nt - 2)
        def _():
            copy = hop(0, end_t, k)
            copy.wait_recv()
            copy.start()

        hop(1, other_mid, k).wait_recv()
        hop(1, other_end, k).wait_recv()
        total = jnp.zeros((length, 1), jnp.float32)
        for s in range(nt):
            wide = gath[s, k].astype(jnp.float32)
            total = total + jnp.sum(wide * wide, axis=1, keepdims=True)
        inverse = lax.rsqrt(total / (features * nt) + 1e-05)
        scales[k] = jnp.broadcast_to(inverse, (length, length)).T[0:1]
        for s in range(nt):
            wide = gath[s, k].astype(jnp.float32)
            scaled = wide * inverse * gains[s].astype(jnp.float32)
            at = (s % (nt // 2)) * features
            normed[s // (nt // 2), k, :, at:at + features] = scaled.astype(jnp.bfloat16)
        for c in range(0, width, tile):
            part[k, :, c:c + tile] = jnp.dot(
                normed[far, k], weight_end[:, c:c + tile],
                preferred_element_type=jnp.float32,
            ).astype(jnp.bfloat16)
        scale_move(k).start()
        part_move(k).start()

    @pl.when(mid)
    def _():
        wx_out().wait_recv()
        wx_across().start()
        for d in evens:
            @pl.when(in_far(d))
            def _(d=d):
                kvx_direct(d).wait_recv()
                kvx_across(d).start()

        wx_across().wait_recv()
        for d in range(0, n, 2):
            @pl.when(in_far(d))
            def _(d=d):
                kvx_across(d).wait_recv()

        def early(k, carry):
            mid_step(k)
            return carry

        lax.fori_loop(0, n - 2, early, 0)
        relay_kv()
        for copy in wq_loads:
            copy.wait()
        lax.fori_loop(n - 2, n, early, 0)

        def rest(q, carry):
            own_project(q)
            return carry

        lax.fori_loop(0, n // batch, rest, 0)

    @pl.when(end)
    def _():
        relay_kv()
        for copy in wq_loads:
            copy.wait()
        def step(k, carry):
            hop(1, mid_t, k).wait_recv()
            scale_move(k).wait_recv()
            inverse = jnp.broadcast_to(scales[k], (length, length)).T[:, 0:1]
            for i in range(nt // 2):
                s = side * (nt // 2) + i
                wide = gath[s, k].astype(jnp.float32)
                scaled = wide * inverse * gains[s].astype(jnp.float32)
                normed[side, k, :, i * features:(i + 1) * features] = scaled.astype(jnp.bfloat16)
            part_move(k).wait_recv()
            for c in range(0, width, tile):
                projected[k, :, c:c + tile] = (
                    jnp.dot(
                        normed[side, k], weight[side, :, c:c + tile],
                        preferred_element_type=jnp.float32,
                    )
                    + part[k, :, c:c + tile].astype(jnp.float32)
                ).astype(jnp.bfloat16)
            out_copy(k).start()
            return carry

        lax.fori_loop(0, n, step, 0)

    for k in range(1, n):
        swap(k).wait_send()
    for d in evens:
        kv_direct(d).wait_send()
    for d in range(0, n, 2):
        kv_across(d).wait_send()
    for j in range(1, nt):
        gain_move(j).wait_send()

    @pl.when(end)
    def _():
        wx_out().wait_send()

    @pl.when(mid & in_far(0))
    def _():
        for d in evens:
            kvx_direct(d).wait_send()

    @pl.when(mid)
    def _():
        wx_across().wait_send()
        for d in range(0, n, 2):
            @pl.when(in_far(d))
            def _(d=d):
                kvx_across(d).wait_send()

    def drain(k, carry):
        @pl.when(t < nt - 1)
        def _():
            hop(1, t, k).wait_send()

        @pl.when(t > 0)
        def _():
            hop(0, t, k).wait_send()

        @pl.when(t == 1)
        def _():
            hop(1, end_t, k).wait_send()

        @pl.when(t == nt - 2)
        def _():
            hop(0, end_t, k).wait_send()

        @pl.when(mid)
        def _():
            scale_move(k).wait_send()
            part_move(k).wait_send()

        return carry

    lax.fori_loop(0, n, drain, 0)
    for k in range(n):
        out_copy(k).wait()


def attention_kernel(heads_dev, groups_dev, back, places_ref, seg_ref, qkv_ref, out_ref, held, segs, sem):
    r = pl.program_id(0)
    count, length, _ = qkv_ref.shape
    span = (back + 1) * length

    def fetch(k):
        place = places_ref[k]
        return pltpu.make_async_copy(qkv_ref.at[k], held.at[place + back], sem.at[place])

    @pl.when(r == 0)
    def _():
        for k in range(count):
            fetch(k).start()
        held[0:back] = jnp.zeros((back,) + held.shape[1:], held.dtype)
        for k in range(back):
            segs[k] = jnp.full((1, length), -1, jnp.int32)
        for k in range(count):
            segs[back + k] = seg_ref[:, k * length:(k + 1) * length]

    pltpu.make_async_copy(qkv_ref.at[0], held.at[r + back], sem.at[r]).wait()
    own_seg = jnp.broadcast_to(segs[r + back], (length, length)).T
    same = [own_seg == segs[r + b] for b in range(back + 1)]
    rows_i = lax.broadcasted_iota(jnp.int32, (length, length), 0)
    cols_i = lax.broadcasted_iota(jnp.int32, (length, length), 1)
    same[back] = same[back] & (cols_i <= rows_i)
    bias = jnp.concatenate([jnp.where(m, 0.0, -1e30) for m in same], axis=1)
    stack = heads_dev // groups_dev
    bias = jnp.concatenate([bias] * stack, axis=0)
    base = heads_dev * HD
    for g in range(groups_dev):
        first = g * stack
        query = jnp.concatenate(
            [held[r + back, :, (first + i) * HD:(first + i + 1) * HD] for i in range(stack)], axis=0
        )
        k_at = base + 2 * g * HD
        key = jnp.concatenate([held[r + b, :, k_at:k_at + HD] for b in range(back + 1)], axis=0)
        value = jnp.concatenate(
            [held[r + b, :, k_at + HD:k_at + 2 * HD] for b in range(back + 1)], axis=0
        )
        scores = lax.dot_general(
            query, key, (((1,), (1,)), ((), ())), preferred_element_type=jnp.float32
        )
        masked = scores * (1.0 / math.sqrt(HD)) + bias
        top = jnp.max(masked, axis=1, keepdims=True)
        power = jnp.exp(masked - top)
        probs = (power * (1.0 / jnp.sum(power, axis=1, keepdims=True))).astype(jnp.bfloat16)
        context = jnp.dot(probs, value, preferred_element_type=jnp.float32).astype(jnp.bfloat16)
        for i in range(stack):
            out_ref[:, (first + i) * HD:(first + i + 1) * HD] = context[i * length:(i + 1) * length]


def attention(qkv, seg_ids, places, heads_dev, groups_dev):
    count, length, width = qkv.shape
    back = (MAX_RUN - 1 + length - 1) // length
    return pl.pallas_call(
        functools.partial(attention_kernel, heads_dev, groups_dev, back),
        grid_spec=pltpu.PrefetchScalarGridSpec(
            num_scalar_prefetch=1,
            grid=(count,),
            in_specs=[
                pl.BlockSpec(memory_space=pltpu.VMEM),
                pl.BlockSpec(memory_space=pl.ANY),
            ],
            out_specs=pl.BlockSpec((length, heads_dev * HD), lambda r, places: (r, 0)),
            scratch_shapes=[
                pltpu.VMEM((count + back, length, width), jnp.bfloat16),
                pltpu.VMEM((count + back, 1, length), jnp.int32),
                pltpu.SemaphoreType.DMA((count,)),
            ],
        ),
        out_shape=jax.ShapeDtypeStruct((count * length, heads_dev * HD), jnp.bfloat16),
        compiler_params=pltpu.CompilerParams(dimension_semantics=("arbitrary",)),
        name="attention",
    )(places, seg_ids, qkv)


def on_device_pairwise(n, nt, blocks, seg_ids, dest, slot, norm_gain, w_query, w_keyval):
    order = sorted(range(n), key=lambda d: (bin(d).count("1"), d))
    own_index = lax.axis_index("learner")
    blk_dev, block_len, features = blocks.shape
    heads_dev = w_query.shape[1] // HD
    groups_dev = heads_dev // (HEADS // KV_HEADS)
    own_cols = w_query.shape[1]
    kv_cols = groups_dev * 2 * HD
    width = own_cols + kv_cols
    rows = w_query.shape[0]
    any_spec = pl.BlockSpec(memory_space=pl.ANY)
    qkv = pl.pallas_call(
        functools.partial(gather_project_kernel, order, n, nt, own_cols, kv_cols),
        out_shape=jax.ShapeDtypeStruct((n, block_len, width), jnp.bfloat16),
        in_specs=[
            pl.BlockSpec(memory_space=pltpu.SMEM),
            any_spec,
            pl.BlockSpec(memory_space=pltpu.VMEM),
            any_spec,
            any_spec,
        ],
        out_specs=any_spec,
        scratch_shapes=[
            pltpu.VMEM((n, block_len, features), jnp.bfloat16),
            pltpu.VMEM((n, block_len, features), jnp.bfloat16),
            pltpu.VMEM((nt, n, block_len, features), jnp.bfloat16),
            pltpu.VMEM((nt, 1, features), jnp.float32),
            pltpu.VMEM((2, rows // 2, width), jnp.bfloat16),
            pltpu.VMEM((rows // 2, width), jnp.bfloat16),
            pltpu.VMEM((2, n, block_len, rows // 2), jnp.bfloat16),
            pltpu.VMEM((n, block_len, width), jnp.bfloat16),
            pltpu.VMEM((n, block_len, width), jnp.bfloat16),
            pltpu.VMEM((n, 1, block_len), jnp.float32),
        ]
        + [pltpu.SemaphoreType.DMA, pltpu.SemaphoreType.DMA((2,))]
        + [pltpu.SemaphoreType.DMA] * 2
        + [pltpu.SemaphoreType.DMA((n,))] * 8
        + [pltpu.SemaphoreType.DMA((2,))] * 2
        + [pltpu.SemaphoreType.DMA((nt,))] * 2
        + [pltpu.SemaphoreType.DMA((2, nt, n)), pltpu.SemaphoreType.DMA((nt, n))]
        + [pltpu.SemaphoreType.DMA((n,))] * 5,
        compiler_params=pltpu.CompilerParams(
            collective_id=0, has_side_effects=True, vmem_limit_bytes=60000 * 1024
        ),
        name="gather_project",
    )(dest, blocks, norm_gain.astype(jnp.float32)[None, :], w_query, w_keyval)
    targets = dest.reshape(n, blk_dev)
    arriving = jnp.sum(jnp.where(targets == own_index, slot.reshape(n, blk_dev), 0), axis=1)
    sources = own_index ^ jnp.array(order, jnp.int32)
    places = jnp.sum(
        jnp.where(sources[:, None] == jnp.arange(n, dtype=jnp.int32)[None, :], arriving[None, :], 0),
        axis=1,
    ).astype(jnp.int32)
    return attention(qkv, seg_ids, places, heads_dev, groups_dev)


def solution(mesh):
    n, nt = mesh.shape["learner"], mesh.shape["tensor"]

    def on_device(blocks, seg_ids, dest, slot, norm_gain, w_query, w_keyval):
        args = (blocks, seg_ids, dest, slot, norm_gain, w_query, w_keyval)
        whole_groups = w_query.shape[1] % (HD * HEADS // KV_HEADS) == 0
        if blocks.shape[0] == n and n > 2 and n & (n - 1) == 0 and nt == 4 and whole_groups:
            return on_device_pairwise(n, nt, *args)
        return on_device_general(*args)

    return jax.shard_map(
        on_device,
        mesh=mesh,
        in_specs=(
            P("learner", None, "tensor"),
            P("learner", None),
            P(),
            P(),
            P("tensor"),
            P(None, "tensor"),
            P("learner", None),
        ),
        out_specs=P("learner", "tensor"),
        check_vma=False,
    )
```

```python
import functools
import math

import jax
import jax.numpy as jnp
from jax import lax
from jax.experimental import pallas as pl
from jax.experimental.pallas import tpu as pltpu
from jax.sharding import PartitionSpec as P

D = 4096
HEADS = 32
KV_HEADS = 8
HD = 128
MAX_RUN = 256
MESH = pl.DeviceIdType.MESH


def on_device_general(blocks, seg_ids, dest, slot, norm_gain, w_query, w_keyval):
    learners = lax.axis_size("learner")
    own_index = lax.axis_index("learner")
    blk_dev, block_len, features = blocks.shape
    capacity = (blk_dev + learners - 1) // learners
    targets = dest.reshape(learners, blk_dev)
    places = slot.reshape(learners, blk_dev)
    block_ids = jnp.arange(blk_dev, dtype=jnp.int32)
    earlier = block_ids[None, :] < block_ids[:, None]
    same_target = targets[:, :, None] == targets[:, None, :]
    ranks = jnp.sum(jnp.where(same_target & earlier[None], 1, 0), axis=2).astype(jnp.int32)
    own_targets = lax.dynamic_index_in_dim(targets, own_index, 0, keepdims=False)
    own_ranks = lax.dynamic_index_in_dim(ranks, own_index, 0, keepdims=False)
    send_slots = own_targets * capacity + own_ranks
    slot_range = jnp.arange(learners * capacity, dtype=jnp.int32)
    send_table = (send_slots[None, :] == slot_range[:, None]).astype(jnp.bfloat16)
    outgoing = jnp.dot(send_table, blocks.reshape(blk_dev, -1), preferred_element_type=jnp.float32)
    outgoing = outgoing.astype(jnp.bfloat16).reshape(learners * capacity, block_len, features)
    incoming = lax.all_to_all(outgoing, "learner", split_axis=0, concat_axis=0, tiled=True)
    arrive = (targets == own_index).reshape(-1)
    source_slots = (jnp.arange(learners, dtype=jnp.int32)[:, None] * capacity + ranks).reshape(-1)
    place_hot = ((places.reshape(-1)[:, None] == block_ids[None, :]) & arrive[:, None]).astype(
        jnp.float32
    )
    source_hot = (source_slots[:, None] == slot_range[None, :]).astype(jnp.float32)
    receive_table = jnp.dot(place_hot.T, source_hot).astype(jnp.bfloat16)
    local = jnp.dot(
        receive_table, incoming.reshape(learners * capacity, -1), preferred_element_type=jnp.float32
    )
    local = local.astype(jnp.bfloat16).reshape(blk_dev * block_len, features)
    heads_dev = w_query.shape[1] // HD
    per_group = HEADS // KV_HEADS
    groups_dev = max(1, heads_dev // per_group)
    first_group = lax.axis_index("tensor") * heads_dev // per_group
    kv_columns = lax.dynamic_slice_in_dim(w_keyval, first_group * 2 * HD, groups_dev * 2 * HD, 1)
    kv_weight = lax.all_gather(kv_columns, "learner", axis=0, tiled=True)
    own_squares = jnp.einsum("rd,rd->r", local, local, preferred_element_type=jnp.float32)
    squares = lax.psum(own_squares, "tensor")
    inverse_rms = lax.rsqrt(squares / D + 1e-05)
    normed_part = (
        local.astype(jnp.float32) * inverse_rms[:, None] * norm_gain.astype(jnp.float32)[None, :]
    ).astype(jnp.bfloat16)
    part_rows = lax.all_gather(normed_part, "tensor", axis=1, tiled=True)
    query_sum = jnp.dot(part_rows, w_query, preferred_element_type=jnp.float32)
    keyval_sum = jnp.dot(part_rows, kv_weight, preferred_element_type=jnp.float32)
    queries = query_sum.astype(jnp.bfloat16)
    keyval = keyval_sum.astype(jnp.bfloat16)
    row_count = queries.shape[0]
    places_own = jnp.arange(row_count // block_len, dtype=jnp.int32)
    qkv = jnp.concatenate([queries, keyval], axis=1)
    qkv = qkv.reshape(row_count // block_len, block_len, -1)
    return attention(qkv, seg_ids, places_own, heads_dev, groups_dev)


def bit_flip(value, mask):
    out = value
    bit = 1
    while bit <= mask:
        if mask & bit:
            out = out + bit - 2 * bit * lax.rem(lax.div(value, bit), 2)
        bit *= 2
    return out


def gather_project_kernel(
    order, n, nt, own_cols, kv_cols,
    dest_ref, blocks_ref, gain_ref, wq_ref, wkv_ref, out_ref,
    staged, sorted_, gath, gains, weight, weight_end, normed, projected, part, scales,
    load_sem, wq_sem, kvl_sem, kvx_l, a2a_s, a2a_r, kv_s, kv_f, kv_r, kvx_s, kvx_f, kvx_r,
    wx_s, wx_r, g_s, g_r, z_s, z_r, p_s, p_r, i_s, i_r, out_sem,
):
    me = lax.axis_index("learner")
    t = lax.axis_index("tensor")
    features = blocks_ref.shape[2]
    length = blocks_ref.shape[1]
    rows = wkv_ref.shape[0]
    width = weight.shape[2]
    half_rows = weight_end.shape[0]
    core = lax.rem(me, 2)
    mid = (t > 0) & (t < nt - 1)
    end = (t == 0) | (t == nt - 1)
    side = lax.div(t, 2)
    far = 1 - side
    end_t = jnp.where(side == 0, 0, nt - 1)
    mid_t = jnp.where(side == 0, 1, nt - 2)
    other_mid = jnp.where(side == 0, nt - 2, 1)
    other_end = jnp.where(side == 0, nt - 1, 0)
    peer_of = [bit_flip(me, d) for d in range(n)]
    peers = [peer_of[d] for d in order]
    evens = range(2, n, 2)

    load = pltpu.make_async_copy(blocks_ref, staged, load_sem)
    load.start()

    def slab(owner):
        place = pl.multiple_of(lax.rem(owner, n // 2) * rows, 128)
        return weight.at[lax.div(owner, n // 2), pl.ds(place, rows), pl.ds(own_cols, kv_cols)]

    def far_slab(owner):
        place = lax.rem(owner, n // 2)
        return weight_end.at[
            pl.ds(pl.multiple_of(place * rows, 128), rows), pl.ds(own_cols, kv_cols)
        ]

    def in_far(d):
        return lax.div(peer_of[d], n // 2) == far

    kv_local = pltpu.make_async_copy(
        wkv_ref.at[:, pl.ds(pl.multiple_of(t * kv_cols, 128), kv_cols)], slab(me), kvl_sem
    )
    kv_local.start()

    def kvx_local():
        return pltpu.make_async_copy(
            wkv_ref.at[:, pl.ds(pl.multiple_of(end_t * kv_cols, 128), kv_cols)],
            far_slab(me), kvx_l,
        )

    @pl.when(mid & in_far(0))
    def _():
        kvx_local().start()

    wq_loads = [
        pltpu.make_async_copy(
            wq_ref.at[pl.ds(h * half_rows, half_rows), :],
            weight.at[h, :, pl.ds(0, own_cols)], wq_sem.at[h],
        )
        for h in range(2)
    ]
    for copy in wq_loads:
        copy.start()

    barrier = pltpu.get_barrier_semaphore()
    for k in range(1, n):
        pl.semaphore_signal(barrier, inc=1, device_id=(peers[k], t), device_id_type=MESH)
    for j in range(1, nt):
        pl.semaphore_signal(
            barrier, inc=1, device_id=(me, lax.rem(t + j, nt)), device_id_type=MESH
        )

    gains[t] = gain_ref[...]
    load.wait()
    for k in range(n):
        pick = jnp.int32(0)
        for b in range(n):
            pick = jnp.where(dest_ref[me * n + b] == peers[k], b, pick)
        if k == 0:
            gath[t, 0] = staged[pick]
        else:
            sorted_[k] = staged[pick]
    pl.semaphore_wait(barrier, n - 1 + nt - 1)

    def remote(src, dst, send, recv, device):
        return pltpu.make_async_remote_copy(
            src_ref=src, dst_ref=dst, send_sem=send, recv_sem=recv,
            device_id=device, device_id_type=MESH,
        )

    def swap(k):
        return remote(sorted_.at[k], gath.at[t, k], a2a_s.at[k], a2a_r.at[k], (peers[k], t))

    def kv_direct(d):
        return remote(slab(me), slab(me), kv_s.at[d], kv_r.at[d], (peer_of[d], t))

    def kv_across(d):
        held = slab(peer_of[d])
        return remote(held, held, kv_f.at[d], kv_r.at[d + 1], (peer_of[1], t))

    def kvx_direct(d):
        return remote(far_slab(me), far_slab(me), kvx_s.at[d], kvx_r.at[d], (peer_of[d], t))

    def kvx_across(d):
        held = far_slab(peer_of[d])
        return remote(held, held, kvx_f.at[d], kvx_r.at[d + 1], (peer_of[1], t))

    def wx_rows(c):
        count = half_rows // 2
        return weight_end.at[pl.ds(pl.multiple_of(c * count, 128), count), pl.ds(0, own_cols)]

    def wx_out():
        count = half_rows // 2
        first = pl.multiple_of(far * half_rows + core * count, 128)
        return remote(
            wq_ref.at[pl.ds(first, count), :], wx_rows(core), wx_s.at[0], wx_r.at[0], (me, mid_t)
        )

    def wx_across():
        held = wx_rows(core)
        return remote(held, held, wx_s.at[1], wx_r.at[1], (peer_of[1], t))

    def gain_move(j):
        return remote(gains.at[t], gains.at[t], g_s.at[j], g_r.at[j], (me, lax.rem(t + j, nt)))

    def hop(way, s, k):
        held = gath.at[s, k]
        return remote(
            held, held, z_s.at[way, s, k], z_r.at[s, k], (me, t + 1 if way else t - 1)
        )

    def part_move(k):
        return remote(part.at[k], part.at[k], p_s.at[k], p_r.at[k], (me, end_t))

    def scale_move(k):
        return remote(scales.at[k], scales.at[k], i_s.at[k], i_r.at[k], (me, end_t))

    @pl.when(end)
    def _():
        wx_out().start()

    for k in range(1, n):
        swap(k).start()
    for j in range(1, nt):
        gain_move(j).start()

    def send_own(k):
        @pl.when(t < nt - 1)
        def _():
            hop(1, t, k).start()

        @pl.when(t > 0)
        def _():
            hop(0, t, k).start()

    @pl.when(mid)
    def _():
        send_own(0)

    @pl.when(mid & in_far(0))
    def _():
        kvx_local().wait()
        for d in evens:
            kvx_direct(d).start()
        kvx_across(0).start()

    kv_local.wait()
    for d in evens:
        kv_direct(d).start()
    kv_across(0).start()

    @pl.when(end)
    def _():
        wx_out().wait_send()
        send_own(0)

    for k in range(1, n):
        swap(k).wait_recv()
        send_own(k)
    for j in range(1, nt):
        gain_move(j).wait_recv()

    tile = 512

    def out_copy(k):
        return pltpu.make_async_copy(projected.at[k], out_ref.at[k], out_sem.at[k])

    def relay_kv():
        for d in evens:
            kv_direct(d).wait_recv()
            kv_across(d).start()
        for d in range(0, n, 2):
            kv_across(d).wait_recv()

    batch = n // 2

    def own_project(q):
        group = pl.ds(q * batch, batch)
        for c in range(0, width, tile):
            low = jnp.dot(
                normed[0, group].reshape(batch * length, half_rows), weight[0, :, c:c + tile],
                preferred_element_type=jnp.float32,
            )
            high = jnp.dot(
                normed[1, group].reshape(batch * length, half_rows), weight[1, :, c:c + tile],
                preferred_element_type=jnp.float32,
            )
            projected[group, :, c:c + tile] = (
                (low + high).astype(jnp.bfloat16).reshape(batch, length, tile)
            )
        for i in range(batch):
            out_copy(q * batch + i).start()

    def mid_step(k):
        @pl.when(t == 1)
        def _():
            copy = hop(1, end_t, k)
            copy.wait_recv()
            copy.start()

        @pl.when(t == nt - 2)
        def _():
            copy = hop(0, end_t, k)
            copy.wait_recv()
            copy.start()

        hop(1, other_mid, k).wait_recv()
        hop(1, other_end, k).wait_recv()
        total = jnp.zeros((length, 1), jnp.float32)
        for s in range(nt):
            wide = gath[s, k].astype(jnp.float32)
            total = total + jnp.sum(wide * wide, axis=1, keepdims=True)
        inverse = lax.rsqrt(total / (features * nt) + 1e-05)
        scales[k] = jnp.broadcast_to(inverse, (length, length)).T[0:1]
        for s in range(nt):
            wide = gath[s, k].astype(jnp.float32)
            scaled = wide * inverse * gains[s].astype(jnp.float32)
            at = (s % (nt // 2)) * features
            normed[s // (nt // 2), k, :, at:at + features] = scaled.astype(jnp.bfloat16)
        for c in range(0, width, tile):
            part[k, :, c:c + tile] = jnp.dot(
                normed[far, k], weight_end[:, c:c + tile],
                preferred_element_type=jnp.float32,
            ).astype(jnp.bfloat16)
        scale_move(k).start()
        part_move(k).start()

    @pl.when(mid)
    def _():
        wx_out().wait_recv()
        wx_across().start()
        for d in evens:
            @pl.when(in_far(d))
            def _(d=d):
                kvx_direct(d).wait_recv()
                kvx_across(d).start()

        wx_across().wait_recv()
        for d in range(0, n, 2):
            @pl.when(in_far(d))
            def _(d=d):
                kvx_across(d).wait_recv()

        def early(k, carry):
            mid_step(k)
            return carry

        lax.fori_loop(0, n - 2, early, 0)
        relay_kv()
        for copy in wq_loads:
            copy.wait()
        lax.fori_loop(n - 2, n, early, 0)

        def rest(q, carry):
            own_project(q)
            return carry

        lax.fori_loop(0, n // batch, rest, 0)

    @pl.when(end)
    def _():
        relay_kv()
        for copy in wq_loads:
            copy.wait()
        def step(k, carry):
            hop(1, mid_t, k).wait_recv()
            scale_move(k).wait_recv()
            inverse = jnp.broadcast_to(scales[k], (length, length)).T[:, 0:1]
            for i in range(nt // 2):
                s = side * (nt // 2) + i
                wide = gath[s, k].astype(jnp.float32)
                scaled = wide * inverse * gains[s].astype(jnp.float32)
                normed[side, k, :, i * features:(i + 1) * features] = scaled.astype(jnp.bfloat16)
            part_move(k).wait_recv()
            for c in range(0, width, tile):
                projected[k, :, c:c + tile] = (
                    jnp.dot(
                        normed[side, k], weight[side, :, c:c + tile],
                        preferred_element_type=jnp.float32,
                    )
                    + part[k, :, c:c + tile].astype(jnp.float32)
                ).astype(jnp.bfloat16)
            out_copy(k).start()
            return carry

        lax.fori_loop(0, n, step, 0)

    for k in range(1, n):
        swap(k).wait_send()
    for d in evens:
        kv_direct(d).wait_send()
    for d in range(0, n, 2):
        kv_across(d).wait_send()
    for j in range(1, nt):
        gain_move(j).wait_send()

    @pl.when(mid & in_far(0))
    def _():
        for d in evens:
            kvx_direct(d).wait_send()

    @pl.when(mid)
    def _():
        wx_across().wait_send()
        for d in range(0, n, 2):
            @pl.when(in_far(d))
            def _(d=d):
                kvx_across(d).wait_send()

    def drain(k, carry):
        @pl.when(t < nt - 1)
        def _():
            hop(1, t, k).wait_send()

        @pl.when(t > 0)
        def _():
            hop(0, t, k).wait_send()

        @pl.when(t == 1)
        def _():
            hop(1, end_t, k).wait_send()

        @pl.when(t == nt - 2)
        def _():
            hop(0, end_t, k).wait_send()

        @pl.when(mid)
        def _():
            scale_move(k).wait_send()
            part_move(k).wait_send()

        return carry

    lax.fori_loop(0, n, drain, 0)
    for k in range(n):
        out_copy(k).wait()


def attention_kernel(heads_dev, groups_dev, back, places_ref, seg_ref, qkv_ref, out_ref, held, segs, sem):
    r = pl.program_id(0)
    count, length, _ = qkv_ref.shape
    span = (back + 1) * length

    def fetch(k):
        place = places_ref[k]
        return pltpu.make_async_copy(qkv_ref.at[k], held.at[place + back], sem.at[place])

    @pl.when(r == 0)
    def _():
        for k in range(count):
            fetch(k).start()
        held[0:back] = jnp.zeros((back,) + held.shape[1:], held.dtype)
        for k in range(back):
            segs[k] = jnp.full((1, length), -1, jnp.int32)
        for k in range(count):
            segs[back + k] = seg_ref[:, k * length:(k + 1) * length]

    pltpu.make_async_copy(qkv_ref.at[0], held.at[r + back], sem.at[r]).wait()
    own_seg = jnp.broadcast_to(segs[r + back], (length, length)).T
    same = [own_seg == segs[r + b] for b in range(back + 1)]
    rows_i = lax.broadcasted_iota(jnp.int32, (length, length), 0)
    cols_i = lax.broadcasted_iota(jnp.int32, (length, length), 1)
    same[back] = same[back] & (cols_i <= rows_i)
    bias = jnp.concatenate([jnp.where(m, 0.0, -1e30) for m in same], axis=1)
    stack = heads_dev // groups_dev
    bias = jnp.concatenate([bias] * stack, axis=0)
    base = heads_dev * HD
    for g in range(groups_dev):
        first = g * stack
        query = jnp.concatenate(
            [held[r + back, :, (first + i) * HD:(first + i + 1) * HD] for i in range(stack)], axis=0
        )
        k_at = base + 2 * g * HD
        key = jnp.concatenate([held[r + b, :, k_at:k_at + HD] for b in range(back + 1)], axis=0)
        value = jnp.concatenate(
            [held[r + b, :, k_at + HD:k_at + 2 * HD] for b in range(back + 1)], axis=0
        )
        scores = lax.dot_general(
            query, key, (((1,), (1,)), ((), ())), preferred_element_type=jnp.float32
        )
        masked = scores * (1.0 / math.sqrt(HD)) + bias
        top = jnp.max(masked, axis=1, keepdims=True)
        power = jnp.exp(masked - top)
        probs = (power * (1.0 / jnp.sum(power, axis=1, keepdims=True))).astype(jnp.bfloat16)
        context = jnp.dot(probs, value, preferred_element_type=jnp.float32).astype(jnp.bfloat16)
        for i in range(stack):
            out_ref[:, (first + i) * HD:(first + i + 1) * HD] = context[i * length:(i + 1) * length]


def attention(qkv, seg_ids, places, heads_dev, groups_dev):
    count, length, width = qkv.shape
    back = (MAX_RUN - 1 + length - 1) // length
    return pl.pallas_call(
        functools.partial(attention_kernel, heads_dev, groups_dev, back),
        grid_spec=pltpu.PrefetchScalarGridSpec(
            num_scalar_prefetch=1,
            grid=(count,),
            in_specs=[
                pl.BlockSpec(memory_space=pltpu.VMEM),
                pl.BlockSpec(memory_space=pl.ANY),
            ],
            out_specs=pl.BlockSpec((length, heads_dev * HD), lambda r, places: (r, 0)),
            scratch_shapes=[
                pltpu.VMEM((count + back, length, width), jnp.bfloat16),
                pltpu.VMEM((count + back, 1, length), jnp.int32),
                pltpu.SemaphoreType.DMA((count,)),
            ],
        ),
        out_shape=jax.ShapeDtypeStruct((count * length, heads_dev * HD), jnp.bfloat16),
        compiler_params=pltpu.CompilerParams(dimension_semantics=("arbitrary",)),
        name="attention",
    )(places, seg_ids, qkv)


def on_device_pairwise(n, nt, blocks, seg_ids, dest, slot, norm_gain, w_query, w_keyval):
    order = sorted(range(n), key=lambda d: (bin(d).count("1"), d))
    own_index = lax.axis_index("learner")
    blk_dev, block_len, features = blocks.shape
    heads_dev = w_query.shape[1] // HD
    groups_dev = heads_dev // (HEADS // KV_HEADS)
    own_cols = w_query.shape[1]
    kv_cols = groups_dev * 2 * HD
    width = own_cols + kv_cols
    rows = w_query.shape[0]
    any_spec = pl.BlockSpec(memory_space=pl.ANY)
    qkv = pl.pallas_call(
        functools.partial(gather_project_kernel, order, n, nt, own_cols, kv_cols),
        out_shape=jax.ShapeDtypeStruct((n, block_len, width), jnp.bfloat16),
        in_specs=[
            pl.BlockSpec(memory_space=pltpu.SMEM),
            any_spec,
            pl.BlockSpec(memory_space=pltpu.VMEM),
            any_spec,
            any_spec,
        ],
        out_specs=any_spec,
        scratch_shapes=[
            pltpu.VMEM((n, block_len, features), jnp.bfloat16),
            pltpu.VMEM((n, block_len, features), jnp.bfloat16),
            pltpu.VMEM((nt, n, block_len, features), jnp.bfloat16),
            pltpu.VMEM((nt, 1, features), jnp.float32),
            pltpu.VMEM((2, rows // 2, width), jnp.bfloat16),
            pltpu.VMEM((rows // 2, width), jnp.bfloat16),
            pltpu.VMEM((2, n, block_len, rows // 2), jnp.bfloat16),
            pltpu.VMEM((n, block_len, width), jnp.bfloat16),
            pltpu.VMEM((n, block_len, width), jnp.bfloat16),
            pltpu.VMEM((n, 1, block_len), jnp.float32),
        ]
        + [pltpu.SemaphoreType.DMA, pltpu.SemaphoreType.DMA((2,))]
        + [pltpu.SemaphoreType.DMA] * 2
        + [pltpu.SemaphoreType.DMA((n,))] * 8
        + [pltpu.SemaphoreType.DMA((2,))] * 2
        + [pltpu.SemaphoreType.DMA((nt,))] * 2
        + [pltpu.SemaphoreType.DMA((2, nt, n)), pltpu.SemaphoreType.DMA((nt, n))]
        + [pltpu.SemaphoreType.DMA((n,))] * 5,
        compiler_params=pltpu.CompilerParams(
            collective_id=0, has_side_effects=True, vmem_limit_bytes=60000 * 1024
        ),
        name="gather_project",
    )(dest, blocks, norm_gain.astype(jnp.float32)[None, :], w_query, w_keyval)
    targets = dest.reshape(n, blk_dev)
    arriving = jnp.sum(jnp.where(targets == own_index, slot.reshape(n, blk_dev), 0), axis=1)
    sources = own_index ^ jnp.array(order, jnp.int32)
    places = jnp.sum(
        jnp.where(sources[:, None] == jnp.arange(n, dtype=jnp.int32)[None, :], arriving[None, :], 0),
        axis=1,
    ).astype(jnp.int32)
    return attention(qkv, seg_ids, places, heads_dev, groups_dev)


def solution(mesh):
    n, nt = mesh.shape["learner"], mesh.shape["tensor"]

    def on_device(blocks, seg_ids, dest, slot, norm_gain, w_query, w_keyval):
        args = (blocks, seg_ids, dest, slot, norm_gain, w_query, w_keyval)
        whole_groups = w_query.shape[1] % (HD * HEADS // KV_HEADS) == 0
        if blocks.shape[0] == n and n > 2 and n & (n - 1) == 0 and nt == 4 and whole_groups:
            return on_device_pairwise(n, nt, *args)
        return on_device_general(*args)

    return jax.shard_map(
        on_device,
        mesh=mesh,
        in_specs=(
            P("learner", None, "tensor"),
            P("learner", None),
            P(),
            P(),
            P("tensor"),
            P(None, "tensor"),
            P("learner", None),
        ),
        out_specs=P("learner", "tensor"),
        check_vma=False,
    )
```
